32 devices in a mesh: prow: 8 (over z, y), pcol: 4 (over x, core).
Axes of the slice: x: 2, y: 2, z: 4, core: 2. Of those that a mesh axis runs over, the one named last changes fastest.
Arguments:
- iface_tiles: int32 [32, 16], replicated, may hold values from 0 to 63, as said below
- interior_sizes: int32 [32], P(('prow', 'pcol')), may hold values from 128 to 512
- coupling: float32 [32, 512, 2048], P(('prow', 'pcol')), may hold values from -0.25 to 0.25
- factor_inverse: float32 [32, 512, 512], P(('prow', 'pcol')), as said below
- interface_block: float32 [8, 8, 4, 16, 128, 128], P('prow', None, 'pcol'), as said below
Outputs:
- schur: float32 [8, 8, 4, 16, 128, 128], P('prow', None, 'pcol')
- panel: float32 [8, 8, 128, 128], P('prow', None, 'pcol')
The draws below stay inside these ranges and needn't reach their ends.
Inputs may be any that keep to these rules, and one draw needn't show every extreme that they name: `iface_tiles`: each row holds 16 distinct tile numbers; for every r, exactly 2 of them are r modulo 8; every tile number stands in exactly 8 rows. `factor_inverse`: each matrix is lower triangular with a diagonal between 0.25 and 1. `interface_block`: diagonal entries lie between 80 and 160; other entries are of order one.
All inputs are finite; a program needn't handle non-finite values.
Results may differ from the reference program's by a relative error of at most 0.0001.
Values sent between devices are 32-bit elements; how exact they have to be, the bound alone decides.
A program may use at most 128 MiB of HBM per device.

```python
import jax
import jax.numpy as jnp
from jax import lax

IFACE = 2048
TILE = 128
NI = 512
LR_DEV = 8
GT = 16
NT = 64
LC = 16
SUBDOMAINS = 32
N_PROW = 8
N_PCOL = 4


def shuffle_row(row_key, values):
    return jax.random.permutation(row_key, values)


def draw_iface_tiles(key, part):
    rows_per = IFACE // TILE // N_PROW
    key_list = jax.random.split(jax.random.fold_in(key, 11), N_PROW)
    orders = jax.vmap(shuffle_row)(key_list, jnp.broadcast_to(jnp.arange(SUBDOMAINS, dtype=jnp.int32), (N_PROW, SUBDOMAINS)))
    quotient = (rows_per * orders.T[:, :, None] + jnp.arange(rows_per, dtype=jnp.int32)[None, None, :]) % LR_DEV
    tile_ids = quotient * N_PROW + jnp.arange(N_PROW, dtype=jnp.int32)[None, :, None]
    tile_ids = tile_ids.reshape(SUBDOMAINS, rows_per * N_PROW).astype(jnp.int32)
    shuffle_keys = jax.random.split(jax.random.fold_in(key, 12), SUBDOMAINS)
    return jax.vmap(shuffle_row)(shuffle_keys, tile_ids).astype(jnp.int32)


def draw_factor_inverse(key, part):
    first_key = jax.random.fold_in(key, 21)
    second_key = jax.random.fold_in(key, 22)
    shape = (SUBDOMAINS, NI, NI)
    noise = jax.random.normal(first_key, shape, jnp.float32) * (0.5 / NI ** 0.5)
    diagonal = jax.random.uniform(second_key, (SUBDOMAINS, NI), jnp.float32, 0.5, 1.0)
    lower = jnp.tril(noise, -1)
    eye_mask = jnp.eye(NI, dtype=jnp.float32)[None, :, :]
    return (lower + eye_mask * diagonal[:, :, None]).astype(jnp.float32)


def draw_interface_block(key, part):
    local_cols = LR_DEV * N_PROW // N_PCOL
    shape = (N_PROW, LR_DEV, N_PCOL, local_cols, TILE, TILE)
    first_key = jax.random.fold_in(key, 31)
    second_key = jax.random.fold_in(key, 32)
    noise = jax.random.normal(first_key, shape, jnp.float32) * 0.5
    diagonal = jax.random.uniform(second_key, shape, jnp.float32, 80.0, 160.0)
    prow_ids = jnp.arange(N_PROW, dtype=jnp.int32)[:, None, None, None, None, None]
    row_tiles = jnp.arange(LR_DEV, dtype=jnp.int32)[None, :, None, None, None, None]
    pcol_ids = jnp.arange(N_PCOL, dtype=jnp.int32)[None, None, :, None, None, None]
    col_tiles = jnp.arange(local_cols, dtype=jnp.int32)[None, None, None, :, None, None]
    inner_rows = jnp.arange(TILE, dtype=jnp.int32)[None, None, None, None, :, None]
    inner_cols = jnp.arange(TILE, dtype=jnp.int32)[None, None, None, None, None, :]
    global_row = (row_tiles * N_PROW + prow_ids) * TILE + inner_rows
    global_col = (col_tiles * N_PCOL + pcol_ids) * TILE + inner_cols
    return jnp.where(global_row == global_col, diagonal, noise).astype(jnp.float32)


def set_ends(entries, stream_key, low, top_value):
    shape = entries.shape
    place = [jax.random.randint(jax.random.fold_in(stream_key, axis), (), 0, shape[axis]) for axis in range(len(shape))]
    entries = entries.at[tuple(place)].set(low)
    longest = shape.index(max(shape))
    place[longest] = (place[longest] + 1) % shape[longest]
    return entries.at[tuple(place)].set(top_value)


def block_scale(stream_key, extent, pieces, smallest, top_value):
    def one(position, shards_of):
        heights = jax.random.uniform(jax.random.fold_in(jax.random.fold_in(stream_key, 6), position), (shards_of,), jnp.float32, smallest / len(pieces), top_value / len(pieces))
        return jnp.repeat(jnp.exp(heights), extent[position] // shards_of).reshape((-1,) + (1,) * (len(extent) - position - 1))

    loudness = one(*pieces[0])
    for cut in pieces[1:]:
        loudness = loudness * one(*cut)
    return loudness


def centred(key, extent, deviation, limit, shards=(), kind=jnp.bfloat16):
    gain = block_scale(key, extent, shards, -0.22, 0.18) if shards else 1.0
    array = jax.random.normal(key, extent, jnp.float32) * deviation * gain
    return jnp.minimum(jnp.maximum(array, -limit), limit).astype(kind)


def setup_inputs(seed: int = 0) -> dict:
    key_of = jax.random.split(jax.random.key(seed), 6)
    iface_tiles = draw_iface_tiles(jax.random.fold_in(key_of[5], 71), 0)
    interior_sizes = set_ends(jax.random.randint(key_of[1], (SUBDOMAINS,), NI // 4, NI + 1), jax.random.fold_in(key_of[1], 1), NI // 4, NI).astype(jnp.int32)
    coupling = centred(key_of[2], (SUBDOMAINS, NI, IFACE), NI ** -0.5, 0.25, ((0, 32),), jnp.float32)
    factor_inverse = draw_factor_inverse(jax.random.fold_in(key_of[5], 71), 0)
    interface_block = draw_interface_block(jax.random.fold_in(key_of[5], 71), 0)
    return {"iface_tiles": iface_tiles, "interior_sizes": interior_sizes, "coupling": coupling, "factor_inverse": factor_inverse, "interface_block": interface_block}


def reference(iface_tiles, interior_sizes, coupling, factor_inverse, interface_block):
    grid_tiles = interface_block.transpose(1, 0, 3, 2, 4, 5).reshape(NT, NT, TILE, TILE)

    def add_domain(index, running):
        live_count = interior_sizes[index]
        row_live = (jnp.arange(NI, dtype=jnp.int32) < live_count)[:, None]
        masked = jnp.where(row_live, coupling[index], 0.0)
        weighted = jnp.dot(factor_inverse[index].astype(jnp.float32), masked.astype(jnp.float32), precision=lax.Precision.HIGHEST, preferred_element_type=jnp.float32)
        weighted = jnp.where(row_live, weighted, 0.0)
        gram = jnp.dot(weighted.T.astype(jnp.float32), weighted.astype(jnp.float32), precision=lax.Precision.HIGHEST, preferred_element_type=jnp.float32)
        tiled = gram.reshape(GT, TILE, GT, TILE).transpose(0, 2, 1, 3)
        tile_ids = iface_tiles[index].astype(jnp.int32)
        return running.at[tile_ids[:, None], tile_ids[None, :]].add(-tiled)
    grid_tiles = lax.fori_loop(0, SUBDOMAINS, add_domain, grid_tiles)
    schur = grid_tiles.reshape(LR_DEV, N_PROW, LC, N_PCOL, TILE, TILE).transpose(1, 0, 3, 2, 4, 5)
    column = grid_tiles[:, 0]
    diag_block = column[0]
    lower = jnp.linalg.cholesky(0.5 * (diag_block + diag_block.T))
    flat = column.reshape(NT * TILE, TILE)
    solved = jax.scipy.linalg.solve_triangular(lower, flat.T, lower=True)
    panel = solved.T.reshape(LR_DEV, N_PROW, TILE, TILE).transpose(1, 0, 2, 3)
    return (schur, panel)
```

```python
import functools

import jax
import jax.numpy as jnp
from jax import lax
from jax.experimental import pallas as pl
from jax.experimental.pallas import tpu as pltpu
from jax.sharding import Mesh, PartitionSpec as P

HIGHEST = lax.Precision.HIGHEST


def split(x):
    high = x.astype(jnp.bfloat16)
    low = (x - high.astype(jnp.float32)).astype(jnp.bfloat16)
    return high, low


def dot3(a_high, a_low, b_high, b_low):
    dot = functools.partial(jnp.dot, preferred_element_type=jnp.float32)
    return dot(a_high, b_high) + (dot(a_high, b_low) + dot(a_low, b_high))


def weigh_kernel(info, factor_ref, left_ref, right_ref, out_ref, high_ref, low_ref):
    @pl.when(pl.program_id(0) == 0)
    def _():
        high, low = split(factor_ref[...])
        high_ref[...] = high
        low_ref[...] = low

    block = jnp.concatenate([left_ref[...], right_ref[...]], axis=1)
    live = lax.broadcasted_iota(jnp.int32, block.shape, 0) < info[0]
    high, low = split(jnp.where(live, block, 0.0))
    product = dot3(high_ref[...], low_ref[...], high, low)
    out_ref[...] = jnp.where(live, product, 0.0)


def weigh(info, factor, coupling, width):
    interior, iface = coupling.shape
    pairs = iface // width // 2
    return pl.pallas_call(
        weigh_kernel,
        grid_spec=pltpu.PrefetchScalarGridSpec(
            num_scalar_prefetch=1,
            grid=(pairs,),
            in_specs=[
                pl.BlockSpec((interior, interior), lambda i, info: (0, 0)),
                pl.BlockSpec((interior, width), lambda i, info: (0, info[1 + 2 * i])),
                pl.BlockSpec((interior, width), lambda i, info: (0, info[2 + 2 * i])),
            ],
            out_specs=pl.BlockSpec((interior, 2 * width), lambda i, info: (0, i)),
            scratch_shapes=[pltpu.VMEM((interior, interior), jnp.bfloat16)] * 2,
        ),
        out_shape=jax.ShapeDtypeStruct((interior, iface), jnp.float32),
        compiler_params=pltpu.CompilerParams(vmem_limit_bytes=24 << 20),
        cost_estimate=pl.CostEstimate(
            flops=6 * interior * interior * iface, bytes_accessed=8 * interior * iface, transcendentals=0
        ),
        name="weigh",
    )(info, factor, coupling, coupling)


def gram_kernel(rows_grid, cols_grid, width, half_ref, w_ref, out_ref, high_ref, low_ref):
    step = pl.program_id(0)
    iface = w_ref.shape[1]
    block = iface // rows_grid
    rows_per = block // width

    @pl.when(step == 0)
    def _():
        for m in range(rows_grid):
            high, low = split(w_ref[:, m * block : (m + 1) * block])
            high_ref[:, m * block : (m + 1) * block] = high
            low_ref[:, m * block : (m + 1) * block] = low

    own = half_ref[0] * (rows_grid // 2) + step
    rows = w_ref[:, pl.ds(pl.multiple_of(own * block, block), block)]
    row_high, row_low = split(rows.T)
    for m in range(rows_grid):
        q, lap = m % cols_grid, m // cols_grid
        cols = slice(m * block, (m + 1) * block)
        product = dot3(row_high, row_low, high_ref[:, cols], low_ref[:, cols])
        for r in range(rows_per):
            for c in range(rows_per):
                out_ref[q, r, lap * rows_per + c] = product[
                    r * width : (r + 1) * width, c * width : (c + 1) * width
                ]


def gram(half, weighted, rows_grid, cols_grid, width):
    interior, iface = weighted.shape
    rows_per = iface // width // rows_grid
    cols_per = iface // width // cols_grid
    steps = rows_grid // 2
    return pl.pallas_call(
        functools.partial(gram_kernel, rows_grid, cols_grid, width),
        grid_spec=pltpu.PrefetchScalarGridSpec(
            num_scalar_prefetch=1,
            grid=(steps,),
            in_specs=[pl.BlockSpec((interior, iface), lambda i, half: (0, 0))],
            out_specs=pl.BlockSpec(
                (cols_grid, rows_per, cols_per, width, width), lambda i, half: (i, 0, 0, 0, 0)
            ),
            scratch_shapes=[pltpu.VMEM((interior, iface), jnp.bfloat16)] * 2,
        ),
        out_shape=jax.ShapeDtypeStruct(
            (steps * cols_grid, rows_per, cols_per, width, width), jnp.float32
        ),
        compiler_params=pltpu.CompilerParams(vmem_limit_bytes=32 << 20),
        cost_estimate=pl.CostEstimate(
            flops=3 * interior * iface * iface, bytes_accessed=4 * interior * iface + 2 * iface * iface, transcendentals=0
        ),
        name="gram",
    )(half, weighted)


def subtract_kernel(slots, base_ref, parts_ref, out_ref):
    step = pl.program_id(0)

    @pl.when(step == 0)
    def _():
        def take(i, carry):
            out_ref[i] = base_ref[i]
            return carry

        lax.fori_loop(0, base_ref.shape[0], take, 0)

    count = parts_ref.shape[1]
    for i in range(count):
        slot = slots[step * count + i]
        out_ref[slot] = out_ref[slot] - parts_ref[0, i]


def subtract(slots, base, parts):
    tiles, width = base.shape[0], base.shape[-1]
    senders, count = parts.shape[:2]
    return pl.pallas_call(
        subtract_kernel,
        grid_spec=pltpu.PrefetchScalarGridSpec(
            num_scalar_prefetch=1,
            grid=(senders,),
            in_specs=[
                pl.BlockSpec((tiles, width, width), lambda i, slots: (0, 0, 0)),
                pl.BlockSpec((1, count, width, width), lambda i, slots: (i, 0, 0, 0)),
            ],
            out_specs=pl.BlockSpec((tiles, width, width), lambda i, slots: (0, 0, 0)),
        ),
        out_shape=jax.ShapeDtypeStruct(base.shape, jnp.float32),
        compiler_params=pltpu.CompilerParams(vmem_limit_bytes=44 << 20),
        cost_estimate=pl.CostEstimate(
            flops=parts.size, bytes_accessed=4 * parts.size + 8 * base.size, transcendentals=0
        ),
        name="subtract",
    )(slots, base, parts)


def shards(iface_tiles, interior_sizes, coupling, factor_inverse, interface_block):
    halves = lax.axis_size("half")
    half_rows = lax.axis_size("sub")
    cols_grid = lax.axis_size("pcol")
    rows_grid = halves * half_rows
    half = lax.axis_index("half")
    prow_index = half * half_rows + lax.axis_index("sub")
    pcol_index = lax.axis_index("pcol")
    self_index = prow_index * cols_grid + pcol_index
    domains, tile_count = iface_tiles.shape
    width = interface_block.shape[-1]
    local_rows, local_cols = interface_block.shape[1], interface_block.shape[3]
    rows_per = tile_count // rows_grid
    cols_per = tile_count // cols_grid
    laps = rows_grid // cols_grid
    share = width // cols_grid
    devices = rows_grid * cols_grid

    order = jnp.argsort(iface_tiles % rows_grid, axis=1, stable=True)
    sorted_tiles = jnp.take_along_axis(iface_tiles, order, axis=1)
    own_order = lax.dynamic_index_in_dim(order, self_index, 0, keepdims=False)
    own_sorted = lax.dynamic_index_in_dim(sorted_tiles, self_index, 0, keepdims=False)
    info = jnp.concatenate([interior_sizes, own_order.astype(jnp.int32)])
    half_info = half.astype(jnp.int32).reshape(1)

    weighted = weigh(info, factor_inverse[0], coupling[0], width)
    across = lax.ppermute(weighted, "half", [(h, (h + 1) % halves) for h in range(halves)])

    own_part = gram(half_info, weighted, rows_grid, cols_grid, width)
    own_received = lax.all_to_all(own_part, ("sub", "pcol"), split_axis=0, concat_axis=0, tiled=True)

    base = interface_block.reshape(local_rows * local_cols, width, width)
    zero_tile = sum(
        jnp.where(own_sorted[r] == 0, weighted[:, r * width : (r + 1) * width], 0.0)
        for r in range(rows_per)
    )
    diag = jnp.where(self_index == 0, base[0], 0.0) - jnp.einsum(
        "kt,ku->tu", zero_tile, zero_tile, precision=HIGHEST
    )
    stride = 1
    while stride < devices:
        axes = ("half", "sub", "pcol")
        diag = diag + lax.ppermute(diag, axes, [(d, d ^ stride) for d in range(devices)])
        stride *= 2
    lower = jnp.linalg.cholesky(0.5 * (diag + diag.T))
    inverse = jax.scipy.linalg.solve_triangular(lower, jnp.eye(width, dtype=jnp.float32), lower=True)

    far_part = gram(half_info, across, rows_grid, cols_grid, width)
    far_received = lax.all_to_all(far_part, ("sub", "pcol"), split_axis=0, concat_axis=0, tiled=True)

    by_row = sorted_tiles.reshape(domains, rows_grid, rows_per)
    target_rows = lax.dynamic_index_in_dim(by_row, prow_index, 1, keepdims=False) // rows_grid
    by_col = sorted_tiles.reshape(domains, laps, cols_grid, rows_per)
    target_cols = lax.dynamic_index_in_dim(by_col, pcol_index, 2, keepdims=False)
    target_cols = target_cols.reshape(domains, cols_per) // cols_grid
    slots = target_rows[:, :, None] * local_cols + target_cols[:, None, :]
    slots = slots.reshape(halves, -1)
    own_slots = lax.dynamic_index_in_dim(slots, half, 0, keepdims=False)
    far_slots = lax.dynamic_index_in_dim(slots, (half + 1) % halves, 0, keepdims=False)

    group = half_rows * cols_grid
    own_received = own_received.reshape(group, rows_per * cols_per, width, width)
    far_received = far_received.reshape(group, rows_per * cols_per, width, width)
    partial = subtract(own_slots, base, own_received)
    summed = subtract(far_slots, partial, far_received)
    schur = summed.reshape(interface_block.shape)

    column = summed.reshape(local_rows, local_cols, width, width)[:, 0]
    kept = jnp.where(pcol_index == 0, column[:, :share], 0.0)
    for q in range(1, cols_grid):
        kept = kept + lax.ppermute(column[:, q * share : (q + 1) * share], "pcol", [(0, q)])
    panel = jnp.einsum("atu,vu->atv", kept, inverse, precision=HIGHEST)
    return (schur, panel[None])


def solution(mesh):
    rows_grid, cols_grid = mesh.shape["prow"], mesh.shape["pcol"]
    grid = Mesh(
        mesh.devices.reshape(2, rows_grid // 2, cols_grid), ("half", "sub", "pcol")
    )
    prow = ("half", "sub")
    every = ("half", "sub", "pcol")
    in_specs = (
        P(),
        P(every),
        P(every, None, None),
        P(every, None, None),
        P(prow, None, "pcol", None, None, None),
    )
    out_specs = (P(prow, None, "pcol", None, None, None), P(prow, None, "pcol", None))
    return jax.shard_map(shards, mesh=grid, in_specs=in_specs, out_specs=out_specs, check_vma=False)
```

```python
import functools

import jax
import jax.numpy as jnp
from jax import lax
from jax.experimental import pallas as pl
from jax.experimental.pallas import tpu as pltpu
from jax.sharding import Mesh, PartitionSpec as P


HIGHEST = lax.Precision.HIGHEST


def split(x):
    high = x.astype(jnp.bfloat16)
    low = (x - high.astype(jnp.float32)).astype(jnp.bfloat16)
    return high, low


def dot3(a_high, a_low, b_high, b_low):
    dot = functools.partial(jnp.dot, preferred_element_type=jnp.float32)
    return dot(a_high, b_high) + (dot(a_high, b_low) + dot(a_low, b_high))


def weigh_kernel(info, factor_ref, left_ref, right_ref, out_ref, high_ref, low_ref):
    @pl.when(pl.program_id(0) == 0)
    def _():
        high, low = split(factor_ref[...])
        high_ref[...] = high
        low_ref[...] = low

    block = jnp.concatenate([left_ref[...], right_ref[...]], axis=1)
    live = lax.broadcasted_iota(jnp.int32, block.shape, 0) < info[0]
    high, low = split(jnp.where(live, block, 0.0))
    product = dot3(high_ref[...], low_ref[...], high, low)
    out_ref[...] = jnp.where(live, product, 0.0)


def weigh(info, factor, coupling, width):
    interior, iface = coupling.shape
    pairs = iface // width // 2
    return pl.pallas_call(
        weigh_kernel,
        grid_spec=pltpu.PrefetchScalarGridSpec(
            num_scalar_prefetch=1,
            grid=(pairs,),
            in_specs=[
                pl.BlockSpec((interior, interior), lambda i, info: (0, 0)),
                pl.BlockSpec((interior, width), lambda i, info: (0, info[1 + 2 * i])),
                pl.BlockSpec((interior, width), lambda i, info: (0, info[2 + 2 * i])),
            ],
            out_specs=pl.BlockSpec((interior, 2 * width), lambda i, info: (0, i)),
            scratch_shapes=[pltpu.VMEM((interior, interior), jnp.bfloat16)] * 2,
        ),
        out_shape=jax.ShapeDtypeStruct((interior, iface), jnp.float32),
        compiler_params=pltpu.CompilerParams(vmem_limit_bytes=62 << 20),
        cost_estimate=pl.CostEstimate(
            flops=6 * interior * interior * iface, bytes_accessed=8 * interior * iface, transcendentals=0
        ),
        name="weigh",
    )(info, factor, coupling, coupling)


def corner_kernel(info, factor_ref, column_ref, base_ref, out_ref):
    block = column_ref[...]
    live = (lax.broadcasted_iota(jnp.int32, block.shape, 0) < info[0]) & (info[2] == 1)
    product = dot3(*split(factor_ref[...]), *split(jnp.where(live, block, 0.0)))
    product = jnp.where(live, product, 0.0)
    square = dot3(*split(product.T), *split(product))
    out_ref[...] = jnp.where(info[3] == 1, base_ref[0], 0.0) - square


def corner(info, factor, coupling, base):
    interior, width = coupling.shape[0], base.shape[-1]
    return pl.pallas_call(
        corner_kernel,
        grid_spec=pltpu.PrefetchScalarGridSpec(
            num_scalar_prefetch=1,
            grid=(1,),
            in_specs=[
                pl.BlockSpec((interior, interior), lambda i, info: (0, 0)),
                pl.BlockSpec((interior, width), lambda i, info: (0, info[1])),
                pl.BlockSpec((1, width, width), lambda i, info: (0, 0, 0)),
            ],
            out_specs=pl.BlockSpec((width, width), lambda i, info: (0, 0)),
        ),
        out_shape=jax.ShapeDtypeStruct((width, width), jnp.float32),
        compiler_params=pltpu.CompilerParams(vmem_limit_bytes=62 << 20),
        cost_estimate=pl.CostEstimate(
            flops=6 * interior * interior * width, bytes_accessed=8 * interior * interior, transcendentals=0
        ),
        name="corner",
    )(info, factor, coupling, base)


def gram_kernel(rows_grid, cols_grid, width, half_ref, w_ref, out_ref, high_ref, low_ref):
    step = pl.program_id(0)
    iface = w_ref.shape[1]
    block = iface // rows_grid
    rows_per = block // width

    @pl.when(step == 0)
    def _():
        for m in range(rows_grid):
            high, low = split(w_ref[:, m * block : (m + 1) * block])
            high_ref[:, m * block : (m + 1) * block] = high
            low_ref[:, m * block : (m + 1) * block] = low

    own = half_ref[0] * (rows_grid // 2) + step
    rows = w_ref[:, pl.ds(pl.multiple_of(own * block, block), block)]
    row_high, row_low = split(rows.T)
    for m in range(rows_grid):
        q, lap = m % cols_grid, m // cols_grid
        cols = slice(m * block, (m + 1) * block)
        product = dot3(row_high, row_low, high_ref[:, cols], low_ref[:, cols])
        for r in range(rows_per):
            for c in range(rows_per):
                out_ref[q, r, lap * rows_per + c] = product[
                    r * width : (r + 1) * width, c * width : (c + 1) * width
                ]


def gram(half, weighted, rows_grid, cols_grid, width):
    interior, iface = weighted.shape
    rows_per = iface // width // rows_grid
    cols_per = iface // width // cols_grid
    steps = rows_grid // 2
    return pl.pallas_call(
        functools.partial(gram_kernel, rows_grid, cols_grid, width),
        grid_spec=pltpu.PrefetchScalarGridSpec(
            num_scalar_prefetch=1,
            grid=(steps,),
            in_specs=[pl.BlockSpec((interior, iface), lambda i, half: (0, 0))],
            out_specs=pl.BlockSpec(
                (cols_grid, rows_per, cols_per, width, width), lambda i, half: (i, 0, 0, 0, 0)
            ),
            scratch_shapes=[pltpu.VMEM((interior, iface), jnp.bfloat16)] * 2,
        ),
        out_shape=jax.ShapeDtypeStruct(
            (steps * cols_grid, rows_per, cols_per, width, width), jnp.float32
        ),
        compiler_params=pltpu.CompilerParams(vmem_limit_bytes=62 << 20),
        cost_estimate=pl.CostEstimate(
            flops=3 * interior * iface * iface, bytes_accessed=4 * interior * iface + 2 * iface * iface, transcendentals=0
        ),
        name="gram",
    )(half, weighted)


def subtract_kernel(slots, base_ref, parts_ref, out_ref):
    step = pl.program_id(0)

    @pl.when(step == 0)
    def _():
        def take(i, carry):
            out_ref[i] = base_ref[i]
            return carry

        lax.fori_loop(0, base_ref.shape[0], take, 0)

    count = parts_ref.shape[1]
    for i in range(count):
        slot = slots[step * count + i]
        out_ref[slot] = out_ref[slot] - parts_ref[0, i]


def subtract(slots, base, parts):
    tiles, width = base.shape[0], base.shape[-1]
    senders, count = parts.shape[:2]
    return pl.pallas_call(
        subtract_kernel,
        grid_spec=pltpu.PrefetchScalarGridSpec(
            num_scalar_prefetch=1,
            grid=(senders,),
            in_specs=[
                pl.BlockSpec((tiles, width, width), lambda i, slots: (0, 0, 0)),
                pl.BlockSpec((1, count, width, width), lambda i, slots: (i, 0, 0, 0)),
            ],
            out_specs=pl.BlockSpec((tiles, width, width), lambda i, slots: (0, 0, 0)),
        ),
        out_shape=jax.ShapeDtypeStruct(base.shape, jnp.float32),
        compiler_params=pltpu.CompilerParams(vmem_limit_bytes=62 << 20),
        cost_estimate=pl.CostEstimate(
            flops=parts.size, bytes_accessed=4 * parts.size + 8 * base.size, transcendentals=0
        ),
        name="subtract",
    )(slots, base, parts)


def assemble(iface_tiles, interior_sizes, coupling, factor_inverse, interface_block):
    halves = lax.axis_size("half")
    half_rows = lax.axis_size("sub")
    cols_grid = lax.axis_size("pcol")
    rows_grid = halves * half_rows
    half = lax.axis_index("half")
    prow_index = half * half_rows + lax.axis_index("sub")
    pcol_index = lax.axis_index("pcol")
    self_index = prow_index * cols_grid + pcol_index
    domains, tile_count = iface_tiles.shape
    width = interface_block.shape[-1]
    local_rows, local_cols = interface_block.shape[1], interface_block.shape[3]
    rows_per = tile_count // rows_grid
    cols_per = tile_count // cols_grid
    laps = rows_grid // cols_grid
    share = width // cols_grid
    devices = rows_grid * cols_grid

    order = jnp.argsort(iface_tiles % rows_grid, axis=1, stable=True)
    sorted_tiles = jnp.take_along_axis(iface_tiles, order, axis=1)
    own_order = lax.dynamic_index_in_dim(order, self_index, 0, keepdims=False)
    info = jnp.concatenate([interior_sizes, own_order.astype(jnp.int32)])
    half_info = half.astype(jnp.int32).reshape(1)

    by_row = sorted_tiles.reshape(domains, rows_grid, rows_per)
    target_rows = lax.dynamic_index_in_dim(by_row, prow_index, 1, keepdims=False) // rows_grid
    by_col = sorted_tiles.reshape(domains, laps, cols_grid, rows_per)
    target_cols = lax.dynamic_index_in_dim(by_col, pcol_index, 2, keepdims=False)
    target_cols = target_cols.reshape(domains, cols_per) // cols_grid
    slots = target_rows[:, :, None] * local_cols + target_cols[:, None, :]
    slots = slots.reshape(halves, -1)
    own_slots = lax.dynamic_index_in_dim(slots, half, 0, keepdims=False)
    far_slots = lax.dynamic_index_in_dim(slots, (half + 1) % halves, 0, keepdims=False)

    base = interface_block.reshape(local_rows * local_cols, width, width)
    own_tiles = lax.dynamic_index_in_dim(iface_tiles, self_index, 0, keepdims=False)
    corner_info = jnp.stack(
        [
            interior_sizes[0],
            jnp.max(jnp.where(own_tiles == 0, lax.iota(jnp.int32, tile_count), 0)),
            jnp.any(own_tiles == 0).astype(jnp.int32),
            (self_index == 0).astype(jnp.int32),
        ]
    )
    diag = corner(corner_info, factor_inverse[0], coupling[0], base)

    def exchange(diag, strides):
        for stride in strides:
            pairs = [(d, d ^ stride) for d in range(devices)]
            diag = diag + lax.ppermute(diag, ("half", "sub", "pcol"), pairs)
        return diag

    strides = [1 << k for k in range(devices.bit_length() - 1)]
    near = half_rows * cols_grid // 4
    diag = exchange(diag, [stride for stride in strides[::-1] if stride > near])
    weighted = weigh(info, factor_inverse[0], coupling[0], width)
    sent, diag = lax.optimization_barrier((weighted, diag))
    across = lax.ppermute(sent, "half", [(h, (h + 1) % halves) for h in range(halves)])
    diag = exchange(diag, [stride for stride in strides if stride <= near])
    own_part = gram(half_info, weighted, rows_grid, cols_grid, width)
    own_part, diag = lax.optimization_barrier((own_part, diag))
    own_received = lax.all_to_all(own_part, ("sub", "pcol"), split_axis=0, concat_axis=0, tiled=True)
    lower = jnp.linalg.cholesky(0.5 * (diag + diag.T))
    inverse = jax.scipy.linalg.solve_triangular(lower, jnp.eye(width, dtype=jnp.float32), lower=True)
    across, inverse, own_slots, far_slots = lax.optimization_barrier((across, inverse, own_slots, far_slots))

    far_part = gram(half_info, across, rows_grid, cols_grid, width)
    far_received = lax.all_to_all(far_part, ("sub", "pcol"), split_axis=0, concat_axis=0, tiled=True)

    group = half_rows * cols_grid
    own_received = own_received.reshape(group, rows_per * cols_per, width, width)
    far_received = far_received.reshape(group, rows_per * cols_per, width, width)
    partial = subtract(own_slots, base, own_received)
    summed = subtract(far_slots, partial, far_received)
    schur = summed.reshape(interface_block.shape)

    column = summed.reshape(local_rows, local_cols, width, width)[:, 0]
    kept = jnp.where(pcol_index == 0, column[:, :share], 0.0)
    for q in range(1, cols_grid):
        kept = kept + lax.ppermute(column[:, q * share : (q + 1) * share], "pcol", [(0, q)])
    panel = jnp.einsum("atu,vu->atv", kept, inverse, precision=HIGHEST)
    return (schur, panel[None])


def solution(mesh):
    rows_grid, cols_grid = mesh.shape["prow"], mesh.shape["pcol"]
    grid = Mesh(
        mesh.devices.reshape(2, rows_grid // 2, cols_grid), ("half", "sub", "pcol")
    )
    prow = ("half", "sub")
    every = ("half", "sub", "pcol")
    in_specs = (
        P(),
        P(every),
        P(every, None, None),
        P(every, None, None),
        P(prow, None, "pcol", None, None, None),
    )
    out_specs = (P(prow, None, "pcol", None, None, None), P(prow, None, "pcol", None))
    return jax.shard_map(assemble, mesh=grid, in_specs=in_specs, out_specs=out_specs, check_vma=False)
```
